32 devices in a mesh: section: 4 (over z), dp: 2 (over y), tensor: 4 (over x, core).
Axes of the slice: x: 2, y: 2, z: 4, core: 2. Of those that a mesh axis runs over, the one named last changes fastest.
Arguments:
- inputs: bfloat16 [8, 2, 64, 2560], P('dp', None, None, ('section', 'tensor')), parts along dimension 0, may hold values from -18 to 18
- sequence_jobs: int32 [8, 2, 1], P('dp'), parts along dimension 0, may hold values from 0 to 3
- entry_sequence: int32 [8], P('dp'), parts along dimension 0, may hold values from 0 to 3, each once
- layer_norm_gain: float32 [4, 2560], P('section'), may hold values from 0.25 to 1.75
- frozen_query_matrix: bfloat16 [4, 2560, 2560], P('section', None, 'tensor'), may hold values from -1 to 1
- frozen_key_matrix: bfloat16 [4, 2560, 2560], P('section', None, 'tensor'), may hold values from -24 to 24
- frozen_value_matrix: bfloat16 [4, 2560, 2560], P('section', None, 'tensor'), may hold values from -0.125 to 0.125
- frozen_output_matrix: bfloat16 [4, 2560, 2560], P('section', 'tensor'), may hold values from -0.125 to 0.125
- adapter_down_maps: bfloat16 [4, 2560, 128], P('section', 'tensor'), may hold values from -0.125 to 0.125
- adapter_up_maps: bfloat16 [4, 2, 64, 2560], P('section', None, None, 'tensor'), may hold values from -1.5 to 1.5
Outputs:
- finished: bfloat16 [8, 2, 64, 2560], P('dp', None, None, ('section', 'tensor')), parts along dimension 0
The draws below stay inside these ranges and needn't reach their ends.
There are 2 independent parts, one for each index of `dp`. The reference program is written for one: setup_inputs(seed, part) draws one part's arguments, and reference() takes and returns one part's arrays. A program takes and returns all parts, laid end to end along the dimension named above; an argument that names none is the same for every part. Nothing has to cross between parts.
Inputs may be any that keep to these rules, and one draw needn't show every extreme that they name: `sequence_jobs`: every one of the 4 jobs owns at least one sequence. `entry_sequence`: a permutation of the 4 micro-batches.
All inputs are finite; a program needn't handle non-finite values.
Results may differ from the reference program's by a relative error of at most 0.039.
Values may be sent and summed in bfloat16 or wider, within the bound.
A program may use at most 64 MiB of HBM per device.

```python
import math
import jax
import jax.numpy as jnp
from jax import lax

MODEL_WIDTH = 2560
HEADS = 20
HEAD_DIM = 128
ADAPTER_RANK = 16
ADAPTER_JOBS = 4
MICRO_SEQUENCES = 2
SEQ = 64
MICRO_BATCHES = 4
WINDOW_LAYERS = 4
N_TENSOR = 4


def shared_projection(key):
    base = jax.random.normal(jax.random.fold_in(key, 11), (WINDOW_LAYERS, MODEL_WIDTH, HEADS * HEAD_DIM), jnp.float32)
    return jnp.clip(base, -6.0, 6.0) / math.sqrt(MODEL_WIDTH)


def draw_frozen_query_matrix(key, part):
    return shared_projection(key).astype(jnp.bfloat16)


def draw_frozen_key_matrix(key, part):
    own_part = jax.random.normal(jax.random.fold_in(key, 12), (WINDOW_LAYERS, MODEL_WIDTH, HEADS * HEAD_DIM), jnp.float32)
    own_part = jnp.clip(own_part, -6.0, 6.0) / math.sqrt(MODEL_WIDTH)
    return own_part.astype(jnp.bfloat16)


def draw_inputs(key, part):
    full_shape = (MICRO_BATCHES, MICRO_SEQUENCES, SEQ, MODEL_WIDTH)
    base = jax.random.normal(jax.random.fold_in(key, 21), full_shape, jnp.float32)
    return jnp.clip(base, -6.0, 6.0).astype(jnp.bfloat16)


def block_levels(own_key, shape, split, least, high):
    def one(position, shards_of):
        draws = jax.random.uniform(jax.random.fold_in(jax.random.fold_in(own_key, 6), position), (shards_of,), jnp.float32, least / len(split), high / len(split))
        return jnp.repeat(jnp.exp(draws), shape[position] // shards_of).reshape((-1,) + (1,) * (len(shape) - position - 1))

    factor_of = one(*split[0])
    for cut in split[1:]:
        factor_of = factor_of * one(*cut)
    return factor_of


def different_ones(key, rows, number_of, top, lift):
    ranking = jax.random.permutation(jax.random.fold_in(key, 1), number_of)
    pull = ranking
    for power in range(3):
        pull = pull * pull // number_of
    pull = pull * lift // number_of
    tickets = jax.random.randint(jax.random.fold_in(key, 2), (rows, number_of), 0, 4096) + pull
    holders = jax.random.permutation(jax.random.fold_in(key, 3), rows)[jnp.arange(number_of) % rows]
    tickets = jnp.where(jnp.arange(rows)[:, None] == holders[None, :], 1 << 14, tickets)
    priority = tickets * number_of + jnp.arange(number_of)
    return lax.top_k(priority.astype(jnp.int32), top)[1].astype(jnp.int32)


def centred(rng, dims, scale, reach, pieces=(), held_as=jnp.bfloat16):
    factor_of = block_levels(rng, dims, pieces, -0.22, 0.18) if pieces else 1.0
    values = jax.random.normal(rng, dims, jnp.float32) * scale * factor_of
    return jnp.minimum(jnp.maximum(values, -reach), reach).astype(held_as)


def setup_inputs(seed: int = 0, part: int = 0) -> dict:
    seeds = jax.random.split(jax.random.key(seed), 11)
    own_keys = jax.random.split(jax.random.fold_in(seeds[10], part), 11)
    return {
        "inputs": draw_inputs(jax.random.fold_in(jax.random.fold_in(seeds[10], part), 71), part),
        "sequence_jobs": different_ones(own_keys[1], MICRO_BATCHES * MICRO_SEQUENCES, ADAPTER_JOBS, 1, 2048).reshape((MICRO_BATCHES, MICRO_SEQUENCES, 1)),
        "entry_sequence": jax.random.permutation(own_keys[2], MICRO_BATCHES).astype(jnp.int32),
        "layer_norm_gain": jnp.clip(1.0 + 0.15 * jax.random.normal(seeds[3], (WINDOW_LAYERS, MODEL_WIDTH), jnp.float32), 0.25, 1.75),
        "frozen_query_matrix": draw_frozen_query_matrix(jax.random.fold_in(seeds[10], 71), part),
        "frozen_key_matrix": draw_frozen_key_matrix(jax.random.fold_in(seeds[10], 71), part),
        "frozen_value_matrix": centred(seeds[6], (WINDOW_LAYERS, MODEL_WIDTH, MODEL_WIDTH), MODEL_WIDTH ** -0.5, 0.125, ((0, 4), (2, 4))),
        "frozen_output_matrix": centred(seeds[7], (WINDOW_LAYERS, MODEL_WIDTH, MODEL_WIDTH), MODEL_WIDTH ** -0.5, 0.125, ((0, 4), (1, 4))),
        "adapter_down_maps": centred(seeds[8], (WINDOW_LAYERS, MODEL_WIDTH, 2 * ADAPTER_JOBS * ADAPTER_RANK), MODEL_WIDTH ** -0.5, 0.125, ((0, 4), (1, 4))),
        "adapter_up_maps": centred(seeds[9], (WINDOW_LAYERS, 2, ADAPTER_JOBS * ADAPTER_RANK, MODEL_WIDTH), ADAPTER_RANK ** -0.5, 1.5, ((0, 4), (3, 4))),
    }


adapter_scale = 2.0

def attend(query_rows, key_vecs, value_rows, head_groupings):
    head_count = query_rows.shape[1] // HEAD_DIM
    grid_shape = (head_groupings, SEQ, head_count, HEAD_DIM)
    q_wide = query_rows.reshape(grid_shape).astype(jnp.float32)
    k_wide = key_vecs.reshape(grid_shape).astype(jnp.float32)
    v_wide = value_rows.reshape(grid_shape).astype(jnp.float32)
    scores = jnp.einsum('bqhd,bkhd->bhqk', q_wide, k_wide) * HEAD_DIM ** (-0.5)
    causal = jnp.arange(SEQ, dtype=jnp.int32)[:, None] >= jnp.arange(SEQ, dtype=jnp.int32)[None, :]
    scores = jnp.where(causal, scores, -jnp.inf)
    row_max = lax.optimization_barrier(jnp.max(scores, axis=-1, keepdims=True))
    weights = jnp.exp(scores - row_max)
    probabilities = (weights / lax.optimization_barrier(jnp.sum(weights, axis=-1, keepdims=True))).astype(jnp.bfloat16)
    mixture = jnp.einsum('bhqk,bkhd->bqhd', probabilities.astype(jnp.float32), v_wide)
    return mixture.astype(jnp.bfloat16).reshape(head_groupings * SEQ, head_count * HEAD_DIM)

def layer_forward(hidden_state, job_per_row, inverse_norm_scale, query_matrix, key_matrix, value_matrix, output_matrix, adapter_lower_part, adapter_upper_part, head_groupings):
    widened = hidden_state.astype(jnp.float32)
    meansq = lax.optimization_barrier(jnp.mean(widened * widened, axis=-1, keepdims=True))
    normalized_input = (widened * lax.rsqrt(meansq + 1e-05) * inverse_norm_scale).astype(jnp.bfloat16)
    lowrank_products = jnp.dot(normalized_input, adapter_lower_part, preferred_element_type=jnp.float32)
    column_job = jnp.arange(lowrank_products.shape[1], dtype=jnp.int32) // ADAPTER_RANK % ADAPTER_JOBS
    lowrank_products = jnp.where(column_job[None, :] == job_per_row[:, None], lowrank_products, 0.0).astype(jnp.bfloat16)
    middle_result = lowrank_products.shape[1] // 2
    query_rows = (jnp.dot(normalized_input, query_matrix, preferred_element_type=jnp.float32) + adapter_scale * jnp.dot(lowrank_products[:, :middle_result], adapter_upper_part[0], preferred_element_type=jnp.float32)).astype(jnp.bfloat16)
    key_vecs = jnp.dot(normalized_input, key_matrix, preferred_element_type=jnp.float32).astype(jnp.bfloat16)
    value_rows = (jnp.dot(normalized_input, value_matrix, preferred_element_type=jnp.float32) + adapter_scale * jnp.dot(lowrank_products[:, middle_result:], adapter_upper_part[1], preferred_element_type=jnp.float32)).astype(jnp.bfloat16)
    heads = attend(query_rows, key_vecs, value_rows, head_groupings)
    rows = heads.shape[0]
    block = MODEL_WIDTH // N_TENSOR
    head_blocks = heads.reshape(rows, N_TENSOR, block).astype(jnp.float32)
    weight_blocks = output_matrix.reshape(N_TENSOR, block, MODEL_WIDTH).astype(jnp.float32)
    partial_value = jnp.einsum('rbf,bfe->bre', head_blocks, weight_blocks).astype(jnp.bfloat16)
    partial_value = lax.optimization_barrier(partial_value)
    summed = lax.optimization_barrier(jnp.sum(partial_value.astype(jnp.float32), axis=0))
    return (widened + summed).astype(jnp.bfloat16)

def reference(inputs, sequence_jobs, entry_sequence, layer_norm_gain, frozen_query_matrix, frozen_key_matrix, frozen_value_matrix, frozen_output_matrix, adapter_down_maps, adapter_up_maps):
    ordered = jnp.take(inputs, entry_sequence, axis=0)
    seq_jobs = jnp.take(sequence_jobs, entry_sequence, axis=0)[:, :, 0]
    job_per_row = jnp.repeat(seq_jobs.reshape(-1), SEQ)
    hidden_state = ordered.reshape(MICRO_BATCHES * MICRO_SEQUENCES * SEQ, MODEL_WIDTH)
    for layer_number in range(WINDOW_LAYERS):
        hidden_state = layer_forward(hidden_state, job_per_row, layer_norm_gain[layer_number], frozen_query_matrix[layer_number], frozen_key_matrix[layer_number], frozen_value_matrix[layer_number], frozen_output_matrix[layer_number], adapter_down_maps[layer_number], adapter_up_maps[layer_number], MICRO_BATCHES * MICRO_SEQUENCES)
    return hidden_state.reshape(MICRO_BATCHES, MICRO_SEQUENCES, SEQ, MODEL_WIDTH)
```

```python
import functools

import jax
import jax.numpy as jnp
from jax import lax
from jax.experimental import pallas as pl
from jax.experimental.pallas import tpu as pltpu
from jax.sharding import PartitionSpec as P

HEAD_DIM = 128
ADAPTER_RANK = 16
ADAPTER_JOBS = 4
ADAPTER_SCALE = 2.0
SEQS_PER_CHUNK = 1

F32 = jnp.float32
BF16 = jnp.bfloat16


def remote(src, dst, send, recv, section, tensor):
    return pltpu.make_async_remote_copy(
        src_ref=src,
        dst_ref=dst,
        send_sem=send,
        recv_sem=recv,
        device_id={"section": section, "tensor": tensor},
        device_id_type=pl.DeviceIdType.MESH,
    )


def kernel(
    S, T, C, CPB, CR, SEQ, F, COL, W, LR,
    entry, jobs, x_ref, gain_ref, wq, wk, wv, wo, d_ref, up_ref,
    out_ref,
    wbuf, obuf, xsel, xin, xh, xn, qkv, heads, pown, psend, precv, xs, zbuf, ostage, orecv,
    w_sem, d_send, d_recv, in_send, in_recv, px_send, px_recv, pp_send, pp_recv,
    f_send, f_recv, r_send, r_recv, x_send, x_recv, z_send, z_recv, o_send, o_recv,
):
    X = T // 2
    H = F // 2
    sec = lax.axis_index("section")
    t = lax.axis_index("tensor")
    c = lax.rem(t, 2)
    x = t // 2
    partner = t + 1 - 2 * c
    nseq = CR // SEQ
    heads_n = COL // HEAD_DIM

    loads = [
        pltpu.make_async_copy(wq.at[0], wbuf.at[:, pl.ds(0, COL)], w_sem.at[0]),
        pltpu.make_async_copy(wk.at[0], wbuf.at[:, pl.ds(COL, COL)], w_sem.at[1]),
        pltpu.make_async_copy(wv.at[0], wbuf.at[:, pl.ds(2 * COL, COL)], w_sem.at[2]),
        pltpu.make_async_copy(wo.at[0, :, pl.ds(0, H)], obuf.at[0], w_sem.at[3]),
        pltpu.make_async_copy(wo.at[0, :, pl.ds(H, H)], obuf.at[1], w_sem.at[4]),
    ]

    for p in range(C):
        xsel[p] = x_ref[entry[p // CPB], (p % CPB) * CR : (p % CPB + 1) * CR, :]

    barrier = pltpu.get_barrier_semaphore()
    me = sec * T + t
    for step in range(1, S * T):
        other = lax.rem(me + step, S * T)
        pl.semaphore_signal(
            barrier,
            inc=1,
            device_id={"section": other // T, "tensor": lax.rem(other, T)},
            device_id_type=pl.DeviceIdType.MESH,
        )
    for load in loads:
        load.start()
    pl.semaphore_wait(barrier, S * T - 1)

    def in_copy(p, from_sec):
        return remote(
            xsel.at[p], xin.at[p, t, from_sec], in_send.at[p], in_recv.at[p, from_sec], 0, t
        )

    @pl.when(sec > 0)
    def _():
        for p in range(C):
            in_copy(p, sec).start()

    @pl.when(sec == 0)
    def _():
        for p in range(C):
            xin[p, t, 0] = xsel[p]

    def d_rows(owner):
        return wbuf.at[pl.ds(pl.multiple_of(owner * COL, COL), COL), pl.ds(3 * COL, LR)]

    def d_peer(k):
        return remote(
            d_ref.at[0], d_rows(t), d_send.at[k], d_recv.at[k], sec, lax.rem(x + k, X) * 2 + c
        )

    def d_own():
        return remote(d_ref.at[0], d_rows(t), d_send.at[0], d_recv.at[0], sec, partner)

    def d_forward(k):
        owner = lax.rem(x - k + X, X) * 2 + c
        return remote(
            d_rows(owner), d_rows(owner), d_send.at[X + k], d_recv.at[X + k], sec, partner
        )

    for k in range(1, X):
        d_peer(k).start()
    d_own().start()
    wbuf[pl.ds(pl.multiple_of(t * COL, COL), COL), 3 * COL :] = d_ref[0]

    def px_copy(p, k):
        return remote(
            xin.at[p, t], xin.at[p, t], px_send.at[p, k], px_recv.at[p, k],
            sec, lax.rem(x + k, X) * 2 + c,
        )

    def pp_copy(p, k):
        owner = lax.rem(x - k + X, X) * 2 + c
        return remote(
            xin.at[p, owner], xin.at[p, owner], pp_send.at[p, k], pp_recv.at[p, k], sec, partner
        )

    def gather_a(p):
        for s in range(1, S):
            in_copy(p, s).wait_recv()
        for k in range(1, X):
            px_copy(p, k).start()
        pp_copy(p, 0).start()

    def gather_b(p):
        for k in range(1, X):
            px_copy(p, k).wait_recv()
            pp_copy(p, k).start()

    def gather_c(p):
        for k in range(X):
            pp_copy(p, k).wait_recv()
        half = S * T // 2
        for piece in range(S * T):
            column = (piece % half) * W
            xh[p, piece // half, :, column : column + W] = xin[p, piece % T, piece // T]

    def forward(p):
        return remote(xh.at[p, c], xh.at[p, c], f_send.at[p], f_recv.at[p], sec, partner)

    def z_copy(p):
        return remote(zbuf.at[p], xh.at[p, c], z_send.at[p], z_recv.at[p], sec + 1, t)

    def r_copy(p):
        return remote(psend.at[p], precv.at[p], r_send.at[p], r_recv.at[p], sec, partner)

    def x_copy(p, k):
        return remote(
            xs.at[p, x], xs.at[p, x], x_send.at[p, k], x_recv.at[p, k],
            sec, lax.rem(x + k, X) * 2 + c,
        )

    def o_copy(p, js, cc):
        return remote(
            ostage.at[p, js * 2 + cc], orecv.at[p], o_send.at[p, js * 2 + cc], o_recv.at[p],
            c * (S // 2) + js, 2 * x + cc,
        )

    causal = lax.broadcasted_iota(jnp.int32, (SEQ, SEQ), 0) >= lax.broadcasted_iota(
        jnp.int32, (SEQ, SEQ), 1
    )
    column_job = lax.broadcasted_iota(jnp.int32, (SEQ, LR), 1) // ADAPTER_RANK % ADAPTER_JOBS

    def front(p):
        halves = [xh[p, h].astype(F32) for h in range(2)]
        ssq = sum(jnp.sum(v * v, axis=-1, keepdims=True) for v in halves)
        scale = lax.rsqrt(ssq * (1.0 / F) + 1e-5)
        for h in range(2):
            xn[:, h * H : (h + 1) * H] = (
                xh[p, h].astype(F32) * scale * gain_ref[:, h * H : (h + 1) * H]
            ).astype(BF16)
        width = wbuf.shape[1]
        block = 512 if width % 512 == 0 else width
        for n in range(0, width, block):
            qkv[:, n : n + block] = jnp.dot(
                xn[...], wbuf[:, n : n + block], preferred_element_type=F32
            )
        for q in range(nseq):
            rows = slice(q * SEQ, (q + 1) * SEQ)
            index = p * nseq + q
            job = jobs[entry[p // CPB], lax.rem(index, CPB * nseq)]
            codes = jnp.where(column_job == job, qkv[rows, 3 * COL :], 0.0).astype(BF16)
            mid = LR // 2
            query = (
                qkv[rows, 0:COL]
                + ADAPTER_SCALE
                * jnp.dot(codes[:, :mid], up_ref[0, 0], preferred_element_type=F32)
            ).astype(BF16)
            keys = qkv[rows, COL : 2 * COL].astype(BF16)
            values = (
                qkv[rows, 2 * COL : 3 * COL]
                + ADAPTER_SCALE
                * jnp.dot(codes[:, mid:], up_ref[0, 1], preferred_element_type=F32)
            ).astype(BF16)
            for h in range(heads_n):
                cols = slice(h * HEAD_DIM, (h + 1) * HEAD_DIM)
                scores = (
                    lax.dot_general(
                        query[:, cols], keys[:, cols], (((1,), (1,)), ((), ())),
                        preferred_element_type=F32,
                    )
                    * HEAD_DIM**-0.5
                )
                scores = jnp.where(causal, scores, -jnp.inf)
                weights = jnp.exp(scores - jnp.max(scores, axis=-1, keepdims=True))
                probs = (weights / jnp.sum(weights, axis=-1, keepdims=True)).astype(BF16)
                heads[rows, cols] = jnp.dot(
                    probs, values[:, cols], preferred_element_type=F32
                ).astype(BF16)
        psend[p] = jnp.dot(heads[...], obuf[1 - c], preferred_element_type=F32).astype(BF16)
        r_copy(p).start()
        pown[...] = jnp.dot(heads[...], obuf[c], preferred_element_type=F32)

    def reduce_pair(p):
        r_copy(p).wait_recv()
        xs[p, x] = (pown[...] + precv[p].astype(F32)).astype(BF16)
        for k in range(1, X):
            x_copy(p, k).start()

    def finish(p):
        for k in range(1, X):
            x_copy(p, k).wait_recv()
        total = xs[p, 0].astype(F32)
        for k in range(1, X):
            total = total + xs[p, k].astype(F32)
        zbuf[p] = (xh[p, c].astype(F32) + total).astype(BF16)

        @pl.when(sec < S - 1)
        def _():
            z_copy(p).start()

        @pl.when(sec == S - 1)
        def _():
            for js in range(S // 2):
                for cc in range(2):
                    for xx in range(X):
                        column = (js * T + 2 * xx + cc) * W

                        @pl.when(x == xx)
                        def _():
                            ostage[p, js * 2 + cc] = zbuf[p, :, column : column + W]

                    mine = jnp.logical_and(c * (S // 2) + js == sec, 2 * x + cc == t)

                    @pl.when(mine)
                    def _():
                        orecv[p] = ostage[p, js * 2 + cc]

                    @pl.when(jnp.logical_not(mine))
                    def _():
                        o_copy(p, js, cc).start()

    @pl.when(sec == 0)
    def _():
        gather_a(0)
        gather_b(0)

    for k in range(1, X):
        d_peer(k).wait_recv()
        d_forward(k).start()
    d_own().wait_recv()
    for k in range(1, X):
        d_forward(k).wait_recv()
    for load in loads:
        load.wait()

    def body(p, carry):
        @pl.when(sec == 0)
        def _():
            @pl.when(p + 1 < C)
            def _():
                gather_a(p + 1)

            gather_c(p)

        @pl.when(sec > 0)
        def _():
            z_copy(p).wait_recv()
            forward(p).start()

        @pl.when(p > 0)
        def _():
            reduce_pair(p - 1)

        @pl.when(sec > 0)
        def _():
            forward(p).wait_recv()

        front(p)

        @pl.when(jnp.logical_and(sec == 0, p + 1 < C))
        def _():
            gather_b(p + 1)

        @pl.when(p > 0)
        def _():
            finish(p - 1)

        return carry

    lax.fori_loop(0, C, body, 0)
    reduce_pair(C - 1)
    finish(C - 1)

    is_local = jnp.logical_and(sec == S - 1, c == 1)

    def drain(p, carry):
        @pl.when(jnp.logical_not(is_local))
        def _():
            o_copy(p, 0, 0).wait_recv()

        out_ref[p] = orecv[p]
        r_copy(p).wait_send()
        for k in range(1, X):
            x_copy(p, k).wait_send()

        @pl.when(sec > 0)
        def _():
            in_copy(p, sec).wait_send()
            forward(p).wait_send()

        @pl.when(sec == 0)
        def _():
            pp_copy(p, 0).wait_send()
            for k in range(1, X):
                px_copy(p, k).wait_send()
                pp_copy(p, k).wait_send()

        @pl.when(sec < S - 1)
        def _():
            z_copy(p).wait_send()

        @pl.when(sec == S - 1)
        def _():
            for js in range(S // 2):
                for cc in range(2):
                    mine = jnp.logical_and(c * (S // 2) + js == sec, 2 * x + cc == t)

                    @pl.when(jnp.logical_not(mine))
                    def _():
                        o_copy(p, js, cc).wait_send()

        return carry

    lax.fori_loop(0, C, drain, 0)
    d_own().wait_send()
    for k in range(1, X):
        d_peer(k).wait_send()
        d_forward(k).wait_send()


def solution(mesh):
    S, T = mesh.shape["section"], mesh.shape["tensor"]

    def shards(inputs, sequence_jobs, entry_sequence, gain, wq, wk, wv, wo, down, up):
        batches, nseq, seq, W = inputs.shape
        F, COL = wq.shape[1], wq.shape[2]
        LR = down.shape[2]
        CR = SEQS_PER_CHUNK * seq
        CPB = nseq // SEQS_PER_CHUNK
        C = batches * CPB
        X, H = T // 2, F // 2
        vmem = pl.BlockSpec(memory_space=pltpu.VMEM)
        smem = pl.BlockSpec(memory_space=pltpu.SMEM)
        anym = pl.BlockSpec(memory_space=pl.ANY)
        dma = pltpu.SemaphoreType.DMA
        out = pl.pallas_call(
            functools.partial(kernel, S, T, C, CPB, CR, seq, F, COL, W, LR),
            out_shape=jax.ShapeDtypeStruct((C, CR, W), BF16),
            in_specs=[smem, smem, vmem, vmem, anym, anym, anym, anym, vmem, vmem],
            out_specs=vmem,
            scratch_shapes=[
                pltpu.VMEM((F, 3 * COL + LR), BF16),
                pltpu.VMEM((2, COL, H), BF16),
                pltpu.VMEM((C, CR, W), BF16),
                pltpu.VMEM((C, T, S, CR, W), BF16),
                pltpu.VMEM((C, 2, CR, H), BF16),
                pltpu.VMEM((CR, F), BF16),
                pltpu.VMEM((CR, 3 * COL + LR), F32),
                pltpu.VMEM((CR, COL), BF16),
                pltpu.VMEM((CR, H), F32),
                pltpu.VMEM((C, CR, H), BF16),
                pltpu.VMEM((C, CR, H), BF16),
                pltpu.VMEM((C, X, CR, H), BF16),
                pltpu.VMEM((C, CR, H), BF16),
                pltpu.VMEM((C, S, CR, W), BF16),
                pltpu.VMEM((C, CR, W), BF16),
                dma((5,)),
                dma((2 * X,)), dma((2 * X,)),
                dma((C,)), dma((C, S)),
                dma((C, X)), dma((C, X)),
                dma((C, X)), dma((C, X)),
                dma((C,)), dma((C,)),
                dma((C,)), dma((C,)),
                dma((C, X)), dma((C, X)),
                dma((C,)), dma((C,)),
                dma((C, S)), dma((C,)),
            ],
            compiler_params=pltpu.CompilerParams(
                collective_id=0, has_side_effects=True, vmem_limit_bytes=60 * 1024 * 1024
            ),
        )(
            entry_sequence, sequence_jobs[:, :, 0], inputs.reshape(batches, nseq * seq, W),
            gain, wq, wk, wv, wo, down, up,
        )
        return out.reshape(batches, nseq, seq, W)

    return jax.shard_map(
        shards,
        mesh=mesh,
        in_specs=(
            P("dp", None, None, ("section", "tensor")),
            P("dp", None, None),
            P("dp"),
            P("section", None),
            P("section", None, "tensor"),
            P("section", None, "tensor"),
            P("section", None, "tensor"),
            P("section", "tensor", None),
            P("section", "tensor", None),
            P("section", None, None, "tensor"),
        ),
        out_specs=P("dp", None, None, ("section", "tensor")),
        check_vma=False,
    )
```

```python
import functools

import jax
import jax.numpy as jnp
from jax import lax
from jax.experimental import pallas as pl
from jax.experimental.pallas import tpu as pltpu
from jax.sharding import PartitionSpec as P

HEAD_DIM = 128
ADAPTER_RANK = 16
ADAPTER_JOBS = 4
ADAPTER_SCALE = 2.0
SEQS_PER_CHUNK = 1
PIECES = 2
IN_FLIGHT = 1

F32 = jnp.float32
BF16 = jnp.bfloat16


def remote(src, dst, send, recv, section, tensor):
    return pltpu.make_async_remote_copy(
        src_ref=src,
        dst_ref=dst,
        send_sem=send,
        recv_sem=recv,
        device_id={"section": section, "tensor": tensor},
        device_id_type=pl.DeviceIdType.MESH,
    )


def packing(W):
    whole, rest = W // 128, W % 128
    return whole, rest, 128 // rest if rest and 128 % rest == 0 else 1


def kernel(
    S, T, C, CPB, CR, SEQ, F, COL, W, LR,
    entry, jobs, x_ref, gain_ref, wq, wk, wv, wo, d_ref, up_ref,
    out_ref,
    wbuf, obuf, xsel, xin, xh, xn, qkv, heads, pown, psend, precv, xs, zbuf, ostage, orecv,
    w_sem, d_send, d_recv, in_send, in_recv, pp_send, pp_recv,
    f_send, f_recv, r_send, r_recv, x_send, x_recv, z_send, z_recv, o_send, o_recv,
):
    X = T // 2
    H = F // 2
    sec = lax.axis_index("section")
    t = lax.axis_index("tensor")
    c = lax.rem(t, 2)
    x = t // 2
    partner = t + 1 - 2 * c
    nseq = CR // SEQ
    heads_n = COL // HEAD_DIM

    loads = [
        pltpu.make_async_copy(wq.at[0], wbuf.at[:, pl.ds(0, COL)], w_sem.at[0]),
        pltpu.make_async_copy(wk.at[0], wbuf.at[:, pl.ds(COL, COL)], w_sem.at[1]),
        pltpu.make_async_copy(wv.at[0], wbuf.at[:, pl.ds(2 * COL, COL)], w_sem.at[2]),
        pltpu.make_async_copy(wo.at[0, :, pl.ds(0, H)], obuf.at[0], w_sem.at[3]),
        pltpu.make_async_copy(wo.at[0, :, pl.ds(H, H)], obuf.at[1], w_sem.at[4]),
    ]

    whole, rest, groups = packing(W)
    RG = CR // groups
    for p in range(C):
        value = x_ref[entry[p // CPB], (p % CPB) * CR : (p % CPB + 1) * CR, :]
        for b in range(whole):
            xsel[p, b * CR : (b + 1) * CR, :128] = value[:, b * 128 : (b + 1) * 128]
        if rest:
            for g in range(groups):
                xsel[p, whole * CR : whole * CR + RG, g * rest : (g + 1) * rest] = value[
                    g * RG : (g + 1) * RG, whole * 128 :
                ]

    barrier = pltpu.get_barrier_semaphore()
    me = sec * T + t
    for step in range(1, S * T):
        other = lax.rem(me + step, S * T)
        pl.semaphore_signal(
            barrier,
            inc=1,
            device_id={"section": other // T, "tensor": lax.rem(other, T)},
            device_id_type=pl.DeviceIdType.MESH,
        )
    for load in loads:
        load.start()
    pl.semaphore_wait(barrier, S * T - 1)

    def in_copy(p, k, from_sec):
        return remote(
            xsel.at[p], xin.at[p, t, from_sec], in_send.at[p, k], in_recv.at[p, k, from_sec],
            0, lax.rem(x + k, X) * 2 + c,
        )

    for p in range(C):

        @pl.when(sec > 0)
        def _():
            if p >= IN_FLIGHT:
                for k in range(X):
                    in_copy(p - IN_FLIGHT, k, sec).wait_send()
            in_copy(p, 0, sec).start()

        @pl.when(sec == 0)
        def _():
            xin[p, t, 0] = xsel[p]

        for k in range(1, X):
            in_copy(p, k, sec).start()

    def d_rows(owner):
        return wbuf.at[pl.ds(pl.multiple_of(owner * COL, COL), COL), pl.ds(3 * COL, LR)]

    def d_peer(k):
        return remote(
            d_ref.at[0], d_rows(t), d_send.at[k], d_recv.at[k], sec, lax.rem(x + k, X) * 2 + c
        )

    def d_own():
        return remote(d_ref.at[0], d_rows(t), d_send.at[0], d_recv.at[0], sec, partner)

    def d_forward(k):
        owner = lax.rem(x - k + X, X) * 2 + c
        return remote(
            d_rows(owner), d_rows(owner), d_send.at[X + k], d_recv.at[X + k], sec, partner
        )

    for k in range(1, X):
        d_peer(k).start()
    d_own().start()
    wbuf[pl.ds(pl.multiple_of(t * COL, COL), COL), 3 * COL :] = d_ref[0]

    def pp_copy(p, k):
        owner = lax.rem(x - k + X, X) * 2 + c
        return remote(
            xin.at[p, owner], xin.at[p, owner], pp_send.at[p, k], pp_recv.at[p, k], sec, partner
        )

    def gather_a(p):
        for k in range(X):
            for s in range(1 if k == 0 else 0, S):
                in_copy(p, k, s).wait_recv()
            pp_copy(p, k).start()

    def gather_c(p):
        for k in range(X):
            pp_copy(p, k).wait_recv()
        half = S * T // 2
        for piece in range(S * T):
            column = (piece % half) * W
            side, owner, level = piece // half, piece % T, piece // T
            for b in range(whole):
                xh[p, side, :, column + b * 128 : column + (b + 1) * 128] = xin[
                    p, owner, level, b * CR : (b + 1) * CR, :128
                ]
            if rest:
                column += whole * 128
                for g in range(groups):
                    xh[p, side, g * RG : (g + 1) * RG, column : column + rest] = xin[
                        p, owner, level, whole * CR : whole * CR + RG, g * rest : (g + 1) * rest
                    ]

    SR = CR // PIECES

    def rows_of(j):
        return pl.ds(j * SR, SR)

    def forward(p, j):
        part = xh.at[p, c, rows_of(j)]
        return remote(part, part, f_send.at[p, j], f_recv.at[p, j], sec, partner)

    def z_copy(p, j):
        return remote(
            zbuf.at[p, rows_of(j)], xh.at[p, c, rows_of(j)], z_send.at[p, j], z_recv.at[p, j],
            sec + 1, t,
        )

    def r_copy(p):
        return remote(psend.at[p], precv.at[p], r_send.at[p], r_recv.at[p], sec, partner)

    def x_copy(p, k, j):
        part = xs.at[p, x, rows_of(j)]
        return remote(
            part, part, x_send.at[p, k, j], x_recv.at[p, k, j],
            sec, lax.rem(x + k, X) * 2 + c,
        )

    def o_copy(p, js, cc):
        return remote(
            ostage.at[p, js * 2 + cc], orecv.at[p], o_send.at[p, js * 2 + cc], o_recv.at[p],
            c * (S // 2) + js, 2 * x + cc,
        )

    causal = lax.broadcasted_iota(jnp.int32, (SEQ, SEQ), 0) >= lax.broadcasted_iota(
        jnp.int32, (SEQ, SEQ), 1
    )
    column_job = lax.broadcasted_iota(jnp.int32, (SEQ, LR), 1) // ADAPTER_RANK % ADAPTER_JOBS

    def front(p):
        halves = [xh[p, h].astype(F32) for h in range(2)]
        ssq = sum(jnp.sum(v * v, axis=-1, keepdims=True) for v in halves)
        scale = lax.rsqrt(ssq * (1.0 / F) + 1e-5)
        for h in range(2):
            xn[:, h * H : (h + 1) * H] = (
                xh[p, h].astype(F32) * scale * gain_ref[:, h * H : (h + 1) * H]
            ).astype(BF16)
        width = wbuf.shape[1]
        block = 512 if width % 512 == 0 else width
        for n in range(0, width, block):
            qkv[:, n : n + block] = jnp.dot(
                xn[...], wbuf[:, n : n + block], preferred_element_type=F32
            )
        for q in range(nseq):
            rows = slice(q * SEQ, (q + 1) * SEQ)
            index = p * nseq + q
            job = jobs[entry[p // CPB], lax.rem(index, CPB * nseq), 0]
            codes = jnp.where(column_job == job, qkv[rows, 3 * COL :], 0.0).astype(BF16)
            mid = LR // 2
            query = (
                qkv[rows, 0:COL]
                + ADAPTER_SCALE
                * jnp.dot(codes[:, :mid], up_ref[0, 0], preferred_element_type=F32)
            ).astype(BF16)
            keys = qkv[rows, COL : 2 * COL].astype(BF16)
            values = (
                qkv[rows, 2 * COL : 3 * COL]
                + ADAPTER_SCALE
                * jnp.dot(codes[:, mid:], up_ref[0, 1], preferred_element_type=F32)
            ).astype(BF16)
            for h in range(heads_n):
                cols = slice(h * HEAD_DIM, (h + 1) * HEAD_DIM)
                scores = (
                    lax.dot_general(
                        query[:, cols], keys[:, cols], (((1,), (1,)), ((), ())),
                        preferred_element_type=F32,
                    )
                    * HEAD_DIM**-0.5
                )
                scores = jnp.where(causal, scores, -jnp.inf)
                weights = jnp.exp(scores - jnp.max(scores, axis=-1, keepdims=True))
                probs = (weights / jnp.sum(weights, axis=-1, keepdims=True)).astype(BF16)
                heads[rows, cols] = jnp.dot(
                    probs, values[:, cols], preferred_element_type=F32
                ).astype(BF16)

    def project(p):
        psend[p] = jnp.dot(heads[...], obuf[1 - c], preferred_element_type=F32).astype(BF16)
        r_copy(p).start()

    def project_own():
        pown[...] = jnp.dot(heads[...], obuf[c], preferred_element_type=F32)

    def reduce_pair(p):
        r_copy(p).wait_recv()
        for j in range(PIECES):
            part = slice(j * SR, (j + 1) * SR)
            xs[p, x, part] = (pown[part] + precv[p, part].astype(F32)).astype(BF16)
            for k in range(1, X):
                x_copy(p, k, j).start()

    def finish(p):
        for j in range(PIECES):
            part = slice(j * SR, (j + 1) * SR)
            for k in range(1, X):
                x_copy(p, k, j).wait_recv()
            total = xs[p, 0, part].astype(F32)
            for k in range(1, X):
                total = total + xs[p, k, part].astype(F32)
            zbuf[p, part] = (xh[p, c, part].astype(F32) + total).astype(BF16)

            @pl.when(sec < S - 1)
            def _():
                z_copy(p, j).start()

        @pl.when(sec == S - 1)
        def _():
            for js in range(S // 2):
                for cc in range(2):
                    for xx in range(X):
                        column = (js * T + 2 * xx + cc) * W

                        @pl.when(x == xx)
                        def _():
                            ostage[p, js * 2 + cc] = zbuf[p, :, column : column + W]

                    mine = jnp.logical_and(c * (S // 2) + js == sec, 2 * x + cc == t)

                    @pl.when(mine)
                    def _():
                        orecv[p] = ostage[p, js * 2 + cc]

                    @pl.when(jnp.logical_not(mine))
                    def _():
                        o_copy(p, js, cc).start()

    @pl.when(sec == 0)
    def _():
        gather_a(0)

    for k in range(1, X):
        d_peer(k).wait_recv()
        d_forward(k).start()
    d_own().wait_recv()
    for k in range(1, X):
        d_forward(k).wait_recv()
    for load in loads:
        load.wait()

    def body(p, carry):
        @pl.when(sec == 0)
        def _():
            gather_c(p)

        @pl.when(sec > 0)
        def _():
            @pl.when(p == 0)
            def _():
                for j in range(PIECES):
                    z_copy(p, j).wait_recv()
                    forward(p, j).start()

            for j in range(PIECES):
                forward(p, j).wait_recv()

        front(p)
        project(p)

        @pl.when(jnp.logical_and(sec == 0, p + 1 < C))
        def _():
            gather_a(p + 1)

        project_own()

        @pl.when(p > 0)
        def _():
            finish(p - 1)

        @pl.when(jnp.logical_and(sec > 0, p + 1 < C))
        def _():
            for j in range(PIECES):
                z_copy(p + 1, j).wait_recv()
                forward(p + 1, j).start()

        reduce_pair(p)
        return carry

    lax.fori_loop(0, C, body, 0)
    finish(C - 1)

    is_local = jnp.logical_and(sec == S - 1, c == 1)

    def drain(p, carry):
        @pl.when(jnp.logical_not(is_local))
        def _():
            o_copy(p, 0, 0).wait_recv()

        out_ref[p] = orecv[p]
        r_copy(p).wait_send()
        for k in range(1, X):
            for j in range(PIECES):
                x_copy(p, k, j).wait_send()

        @pl.when(sec > 0)
        def _():
            for j in range(PIECES):
                forward(p, j).wait_send()

        @pl.when(sec == 0)
        def _():
            for k in range(X):
                pp_copy(p, k).wait_send()
            for k in range(1, X):
                in_copy(p, k, sec).wait_send()

        @pl.when(sec < S - 1)
        def _():
            for j in range(PIECES):
                z_copy(p, j).wait_send()

        @pl.when(sec == S - 1)
        def _():
            for js in range(S // 2):
                for cc in range(2):
                    mine = jnp.logical_and(c * (S // 2) + js == sec, 2 * x + cc == t)

                    @pl.when(jnp.logical_not(mine))
                    def _():
                        o_copy(p, js, cc).wait_send()

        return carry

    lax.fori_loop(0, C, drain, 0)

    @pl.when(sec > 0)
    def _():
        for p in range(max(0, C - IN_FLIGHT), C):
            for k in range(X):
                in_copy(p, k, sec).wait_send()

    d_own().wait_send()
    for k in range(1, X):
        d_peer(k).wait_send()
        d_forward(k).wait_send()


def solution(mesh):
    S, T = mesh.shape["section"], mesh.shape["tensor"]

    def shards(inputs, sequence_jobs, entry_sequence, gain, wq, wk, wv, wo, down, up):
        batches, nseq, seq, W = inputs.shape
        F, COL = wq.shape[1], wq.shape[2]
        LR = down.shape[2]
        CR = SEQS_PER_CHUNK * seq
        CPB = nseq // SEQS_PER_CHUNK
        C = batches * CPB
        X, H = T // 2, F // 2
        whole, rest, groups = packing(W)
        packed = whole * CR + (CR // groups if rest else 0)
        lanes = 128 if whole or groups > 1 else rest
        vmem = pl.BlockSpec(memory_space=pltpu.VMEM)
        smem = pl.BlockSpec(memory_space=pltpu.SMEM)
        anym = pl.BlockSpec(memory_space=pl.ANY)
        dma = pltpu.SemaphoreType.DMA
        out = pl.pallas_call(
            functools.partial(kernel, S, T, C, CPB, CR, seq, F, COL, W, LR),
            out_shape=jax.ShapeDtypeStruct((C, CR, W), BF16),
            in_specs=[smem, smem, vmem, vmem, anym, anym, anym, anym, vmem, vmem],
            out_specs=vmem,
            scratch_shapes=[
                pltpu.VMEM((F, 3 * COL + LR), BF16),
                pltpu.VMEM((2, COL, H), BF16),
                pltpu.VMEM((C, packed, lanes), BF16),
                pltpu.VMEM((C, T, S, packed, lanes), BF16),
                pltpu.VMEM((C, 2, CR, H), BF16),
                pltpu.VMEM((CR, F), BF16),
                pltpu.VMEM((CR, 3 * COL + LR), F32),
                pltpu.VMEM((CR, COL), BF16),
                pltpu.VMEM((CR, H), F32),
                pltpu.VMEM((C, CR, H), BF16),
                pltpu.VMEM((C, CR, H), BF16),
                pltpu.VMEM((C, X, CR, H), BF16),
                pltpu.VMEM((C, CR, H), BF16),
                pltpu.VMEM((C, S, CR, W), BF16),
                pltpu.VMEM((C, CR, W), BF16),
                dma((5,)),
                dma((2 * X,)), dma((2 * X,)),
                dma((C, X)), dma((C, X, S)),
                dma((C, X)), dma((C, X)),
                dma((C, PIECES)), dma((C, PIECES)),
                dma((C,)), dma((C,)),
                dma((C, X, PIECES)), dma((C, X, PIECES)),
                dma((C, PIECES)), dma((C, PIECES)),
                dma((C, S)), dma((C,)),
            ],
            compiler_params=pltpu.CompilerParams(
                collective_id=0, has_side_effects=True, vmem_limit_bytes=60 * 1024 * 1024
            ),
        )(
            entry_sequence, sequence_jobs, inputs.reshape(batches, nseq * seq, W),
            gain, wq, wk, wv, wo, down, up,
        )
        return out.reshape(batches, nseq, seq, W)

    return jax.shard_map(
        shards,
        mesh=mesh,
        in_specs=(
            P("dp", None, None, ("section", "tensor")),
            P("dp", None, None),
            P("dp"),
            P("section", None),
            P("section", None, "tensor"),
            P("section", None, "tensor"),
            P("section", None, "tensor"),
            P("section", "tensor", None),
            P("section", "tensor", None),
            P("section", None, None, "tensor"),
        ),
        out_specs=P("dp", None, None, ("section", "tensor")),
        check_vma=False,
    )
```
